32 devices in a mesh: task: 4 (over z), tile: 8 (over y, x, core).
Axes of the slice: x: 2, y: 2, z: 4, core: 2. Of those that a mesh axis runs over, the one named last changes fastest.
Arguments:
- adjusted: bfloat16 [8, 3584, 18944], P('task', 'tile'), may hold values from -6 to 6
- fisher: bfloat16 [8, 3584, 18944], P('task', 'tile'), may hold values from 0.0099487305 to 10
Outputs:
- merged: bfloat16 [3584, 18944], P(None, ('task', 'tile'))
The draws below stay inside these ranges and needn't reach their ends.
All inputs are finite; a program needn't handle non-finite values.
Results may differ from the reference program's by a relative error of at most 0.001.
Values may be sent and summed in bfloat16 or wider, within the bound.
A program may use at most 256 MiB of HBM per device.

```python
import math
import jax
import jax.numpy as jnp
from jax import lax

D = 3584
FF = 18944
MODELS = 8


def level_of(own_key, extent, cuts, least, top_value):
    def one(position, shards_of):
        steps = jax.random.uniform(jax.random.fold_in(jax.random.fold_in(own_key, 6), position), (shards_of,), jnp.float32, least / len(cuts), top_value / len(cuts))
        return jnp.repeat(jnp.exp(steps), extent[position] // shards_of).reshape((-1,) + (1,) * (len(extent) - position - 1))

    factor_of = one(*cuts[0])
    for cut in cuts[1:]:
        factor_of = factor_of * one(*cut)
    return factor_of


def gaussian(stream_key, dims, width, most, shards=(), dtype=jnp.bfloat16):
    array = width * jax.random.normal(stream_key, dims, jnp.float32)
    if shards:
        array = array * level_of(stream_key, dims, shards, -0.22, 0.18)
    return jnp.clip(array, -most, most).astype(dtype)


def setup_inputs(seed: int = 0) -> dict:
    keys = jax.random.split(jax.random.key(seed), 3)
    adjusted = gaussian(keys[0], (MODELS, D, FF), 1.0, 6.0, ((0, 4), (1, 8)))
    fisher = jnp.clip(jnp.exp(math.log(10.0) - 6.912895 * jax.random.uniform(keys[1], (MODELS, D, FF), jnp.float32) ** level_of(keys[1], (MODELS, D, FF), ((0, 4), (1, 8)), -0.2, 0.2)), 0.0099487305, 10.0).astype(jnp.bfloat16)
    return dict(adjusted=adjusted, fisher=fisher)


def reference(adjusted, fisher):
    def accumulate(carry, pair):
        numerator, denominator = carry
        weights, curvature = pair
        scaled = curvature.astype(jnp.float32)
        return (numerator + scaled * weights.astype(jnp.float32), denominator + scaled), None

    zeros = jnp.zeros((D, FF), jnp.float32)
    (numerator, denominator), unused = lax.scan(accumulate, (zeros, zeros), (adjusted, fisher))
    return (numerator / denominator).astype(jnp.bfloat16)
```

```python
import functools
import math
import jax
import jax.numpy as jnp
from jax import lax
from jax.experimental import pallas as pl
from jax.experimental.pallas import tpu as pltpu
from jax.sharding import PartitionSpec as P

MESH = pl.DeviceIdType.MESH
LANES = 128
LOW, HIGH = 0.0099487305, 10.0
ODD, POWER = 15, 24
LIFT = 2.0**8.25


def over(count, step, carry, unroll=4):
    def trip(i, value):
        for u in range(unroll):
            value = step(i * unroll + u, value)
        return value

    carry = lax.fori_loop(0, count // unroll, trip, carry)
    for j in range(count // unroll * unroll, count):
        carry = step(j, carry)
    return carry


def kernel(n, rows, width, adj, fis, out, from_left, from_right, loc_a, loc_f, wire, got, num, den,
           loc_sem, send_sem, left_sem, right_sem, got_sem):
    me = lax.axis_index("task")
    chunks = out.shape[0] // rows
    blocks = width // LANES
    per_device = adj.shape[0] * math.sqrt(LOW * HIGH)
    f32 = jnp.float32

    def lanes(j, base=0):
        return pl.ds(pl.multiple_of(base + j * LANES, LANES), LANES)

    def loads(s, q, c, slot):
        where = (slice(None), pl.ds(pl.multiple_of(c * rows, rows), rows), pl.ds(pl.multiple_of(q * width, LANES), width))
        return (
            pltpu.make_async_copy(adj.at[where], loc_a.at[s, slot], loc_sem.at[s, slot, 0]),
            pltpu.make_async_copy(fis.at[where], loc_f.at[s, slot], loc_sem.at[s, slot, 1]),
        )

    def sending(s, q, c, slot):
        inbox, sem, to = ((from_left, left_sem, me + 1), (from_right, right_sem, me - 1))[s]
        return pltpu.make_async_remote_copy(
            src_ref=wire.at[s, slot], dst_ref=inbox.at[q, c], send_sem=send_sem.at[s, slot],
            recv_sem=sem.at[q * chunks + c], device_id={"task": to}, device_id_type=MESH)

    def local(s, slot):
        def step(j, carry):
            f, a = loc_f[s, slot, :, :, lanes(j)].astype(f32), loc_a[s, slot, :, :, lanes(j)].astype(f32)
            num[:, lanes(j)] = jnp.sum(f * a, axis=0)
            den[:, lanes(j)] = jnp.sum(f, axis=0)
            return carry

        over(blocks, step, 0)

    def arrive(side, q, c, held):
        sending(side, q, c, 0).wait_recv()
        inbox = (from_left, from_right)[side]
        copy = pltpu.make_async_copy(inbox.at[q, c], got.at[side], got_sem.at[side])
        copy.start()
        copy.wait()
        centre = per_device * held.astype(f32)
        unit = got[side, :, 2 * width:2 * width + LANES].astype(f32) * (1.0 / LIFT)

        def step(j, carry):
            y = got[side, :, lanes(j)].astype(f32)
            d = jnp.exp2(jnp.log2(got[side, :, lanes(j, width)].astype(f32)) * (1.0 / POWER)) * centre
            size = jnp.exp2(jnp.log2(jnp.maximum(jnp.abs(y), 2.0**-126)) * (1.0 / ODD)) * unit
            r = jnp.where(y < 0, -size, jnp.where(y > 0, size, 0.0))
            num[:, lanes(j)] += r * d
            den[:, lanes(j)] += d
            return carry

        over(blocks, step, 0)

    def encode(s, slot, held):
        def ratio(j, top):
            r = num[:, lanes(j)] / den[:, lanes(j)]
            num[:, lanes(j)] = r
            return jnp.maximum(top, jnp.abs(r))

        top = over(blocks, ratio, jnp.zeros((rows, LANES), f32))
        top = jnp.max(top, axis=1, keepdims=True)
        scale = jnp.broadcast_to(jnp.maximum(top * 1.01, 1e-35), (rows, LANES)).astype(jnp.bfloat16)
        wire[s, slot, :, 2 * width:2 * width + LANES] = scale
        factor = LIFT / scale.astype(f32)
        inverse = 1.0 / (per_device * held.astype(f32))

        def step(j, carry):
            x = num[:, lanes(j)] * factor
            x2 = x * x
            x4 = x2 * x2
            x8 = x4 * x4
            wire[s, slot, :, lanes(j)] = ((x * x2) * (x4 * x8)).astype(jnp.bfloat16)
            v = den[:, lanes(j)] * inverse
            v2 = v * v
            v4 = v2 * v2
            v8 = v4 * v4
            wire[s, slot, :, lanes(j, width)] = (v8 * v8 * v8).astype(jnp.bfloat16)
            return carry

        over(blocks, step, 0)

    def finish(c):
        def step(j, carry):
            merged = num[:, lanes(j)] / den[:, lanes(j)]
            out[pl.ds(pl.multiple_of(c * rows, rows), rows), lanes(j)] = merged.astype(jnp.bfloat16)
            return carry

        over(blocks, step, 0)

    has_left, has_right = me > 0, me < n - 1
    barrier = pltpu.get_barrier_semaphore()
    for there, to in ((has_left, me - 1), (has_right, me + 1)):
        @pl.when(there)
        def _():
            pl.semaphore_signal(barrier, inc=1, device_id={"task": to}, device_id_type=MESH)
    pl.semaphore_wait(barrier, has_left.astype(jnp.int32) + has_right.astype(jnp.int32))

    lasts = ((n - 1 - me) * chunks, me * chunks, chunks)
    quarter = (lambda i: n - 1 - i // chunks, lambda i: i // chunks, lambda i: me)

    def begin(s, i):
        for copy in loads(s, quarter[s](i), i % chunks, i % 2):
            copy.start()

    def work(s, i):
        q, c, slot = quarter[s](i), i % chunks, i % 2

        @pl.when(i + 1 < lasts[s])
        def _():
            begin(s, i + 1)

        for copy in loads(s, q, c, slot):
            copy.wait()
        local(s, slot)
        if s != 1:
            @pl.when(has_left)
            def _():
                arrive(0, q, c, me)
        if s != 0:
            @pl.when(has_right)
            def _():
                arrive(1, q, c, n - 1 - me)
        if s == 2:
            finish(c)
            return

        @pl.when(i >= 2)
        def _():
            sending(s, q, c, slot).wait_send()

        encode(s, slot, (me + 1, n - me)[s])
        sending(s, q, c, slot).start()

    for s in range(2):
        @pl.when(lasts[s] > 0)
        def _():
            begin(s, 0)
    begin(2, 0)
    late = (n - 2) * chunks

    def trip(t, carry):
        for s in range(2):
            @pl.when(t < lasts[s])
            def _():
                work(s, t)

        @pl.when(t >= late)
        def _():
            work(2, t - late)
        return carry

    lax.fori_loop(0, late + chunks, trip, 0)
    for s in range(2):
        @pl.when(lasts[s] > 0)
        def _():
            for slot in range(2):
                sending(s, 0, 0, slot).wait_send()


def body(n, adjusted, fisher):
    models, height, columns = adjusted.shape
    width = columns // n
    rows = next(r for r in (32, 16, 8, height) if height % r == 0)
    chunks = height // rows
    bf16 = jnp.bfloat16
    line = 2 * width + LANES
    merged, _, _ = pl.pallas_call(
        functools.partial(kernel, n, rows, width),
        out_shape=(
            jax.ShapeDtypeStruct((height, width), bf16),
            jax.ShapeDtypeStruct((n, chunks, rows, line), bf16),
            jax.ShapeDtypeStruct((n, chunks, rows, line), bf16),
        ),
        in_specs=[pl.BlockSpec(memory_space=pl.ANY)] * 2,
        out_specs=(pl.BlockSpec(memory_space=pltpu.VMEM), pl.BlockSpec(memory_space=pl.ANY), pl.BlockSpec(memory_space=pl.ANY)),
        scratch_shapes=[
            pltpu.VMEM((3, 2, models, rows, width), bf16),
            pltpu.VMEM((3, 2, models, rows, width), bf16),
            pltpu.VMEM((2, 2, rows, line), bf16),
            pltpu.VMEM((2, rows, line), bf16),
            pltpu.VMEM((rows, width), jnp.float32),
            pltpu.VMEM((rows, width), jnp.float32),
            pltpu.SemaphoreType.DMA((3, 2, 2)),
            pltpu.SemaphoreType.DMA((2, 2)),
            pltpu.SemaphoreType.DMA((n * chunks,)),
            pltpu.SemaphoreType.DMA((n * chunks,)),
            pltpu.SemaphoreType.DMA((2,)),
        ],
        compiler_params=pltpu.CompilerParams(collective_id=0, has_side_effects=True, vmem_limit_bytes=60 * 1024 * 1024),
    )(adjusted, fisher)
    return lax.all_to_all(merged, "tile", split_axis=1, concat_axis=0, tiled=True)


def solution(mesh):
    return jax.shard_map(
        functools.partial(body, mesh.shape["task"]),
        mesh=mesh,
        in_specs=(P("task", "tile", None), P("task", "tile", None)),
        out_specs=P(None, ("task", "tile")),
        check_vma=False,
    )
```
